512 devices in a mesh: row: 16 (over y, core), col: 32 (over x, z).
Axes of the slice: x: 4, y: 8, z: 8, core: 2. Of those that a mesh axis runs over, the one named last changes fastest.
Arguments:
- lhat: float32 [4096, 256, 256], P(('row', 'col')), may hold values from -0.375 to 0.375
- ainv_anc: float32 [4096, 256, 256], P(('row', 'col')), may hold values from -1.25 to 1.25
- diag_inv: float32 [32, 256, 256], P('col', 'row'), may hold values from -0.6 to 2, as said below
- targets: int32 [4096, 1], P(('row', 'col')), may hold values from 0 to 31
Outputs:
- diag_blocks: float32 [32, 256, 256], P('col', 'row')
The draws below stay inside these ranges and needn't reach their ends.
Inputs may be any that keep to these rules, and one draw needn't show every extreme that they name: `diag_inv`: each block is lower triangular with its diagonal entries between 0.5 and 2.
All inputs are finite; a program needn't handle non-finite values.
Results may differ from the reference program's by a relative error of at most 0.0003.
Values sent between devices are 32-bit elements; how exact they have to be, the bound alone decides.
A program may use at most 64 MiB of HBM per device.

```python
import jax
import jax.numpy as jnp
from jax import lax

W = 256
H = 256
SN_DEV = 1
SLOT_DEV = 8
SUPER = 32
SLOTS = 4096
N_ROW = 16
N_COL = 32


def draw_diag_inv(key, part):
    first, second = jax.random.split(jax.random.fold_in(key, 17))
    spread = 0.1 * jax.random.normal(first, (SUPER, W, W), jnp.float32)
    spread = jnp.clip(spread, -0.6, 0.6)
    diagonal = jax.random.uniform(second, (SUPER, W), jnp.float32, 0.5, 2.0)
    lower = jnp.tril(spread, -1)
    return lower + diagonal[:, :, None] * jnp.eye(W, dtype=jnp.float32)[None, :, :]


def steps_of(key, extent, shards, least, high):
    factor_of = 1.0
    for dim, shards_of in shards:
        heights = jax.random.uniform(jax.random.fold_in(jax.random.fold_in(key, 6), dim), (shards_of,), jnp.float32, least / len(shards), high / len(shards))
        factor_of = factor_of * jnp.repeat(jnp.exp(heights), extent[dim] // shards_of).reshape((-1,) + (1,) * (len(extent) - 1 - dim))
    return factor_of


def picks_of(own_key, rows, number_of, top, lift):
    ranking = jax.random.permutation(jax.random.fold_in(own_key, 1), number_of)
    boost = ranking
    for power in range(3):
        boost = boost * boost // number_of
    boost = boost * lift // number_of
    tickets = jax.random.randint(jax.random.fold_in(own_key, 2), (rows, number_of), 0, 4096) + boost
    sure = jax.random.permutation(jax.random.fold_in(own_key, 3), rows)[jnp.arange(number_of) % rows]
    tickets = jnp.where(jnp.arange(rows)[:, None] == sure[None, :], 1 << 14, tickets)
    priority = tickets * number_of + jnp.arange(number_of)
    return lax.top_k(priority.astype(jnp.int32), top)[1].astype(jnp.int32)


def normal_values(stream_key, extent, width, bound, shards=(), held_as=jnp.bfloat16):
    drawn = width * jax.random.normal(stream_key, extent, jnp.float32)
    if shards:
        drawn = drawn * steps_of(stream_key, extent, shards, -0.22, 0.18)
    return jnp.clip(drawn, -bound, bound).astype(held_as)


def setup_inputs(seed: int = 0) -> dict:
    key_of = jax.random.split(jax.random.key(seed), 5)
    lhat = normal_values(key_of[0], (SLOTS, H, W), H ** -0.5, 0.375, ((0, 512),), jnp.float32)
    ainv_anc = normal_values(key_of[1], (SLOTS, H, W), ((SN_DEV / (SLOT_DEV * N_ROW)) ** 0.5), 1.25, ((0, 512),), jnp.float32)
    diag_inv = draw_diag_inv(jax.random.fold_in(key_of[4], 71), 0)
    targets = picks_of(key_of[3], SLOTS, SUPER, 1, 512)
    return dict(lhat=lhat, ainv_anc=ainv_anc, diag_inv=diag_inv, targets=targets)


def reference(lhat, ainv_anc, diag_inv, targets):
    group_size = SLOT_DEV * N_COL
    slot_ids = targets[:, 0].reshape(N_ROW, group_size)
    left_all = lhat.reshape(N_ROW, group_size, H, W)
    right_all = ainv_anc.reshape(N_ROW, group_size, H, W)
    labels = jnp.arange(SN_DEV * N_COL, dtype=jnp.int32)

    def accumulate(running, inputs):
        left_blk, right_blk, ids_blk = inputs
        products = jnp.einsum('shi,shj->sij', left_blk, right_blk, precision=lax.Precision.HIGHEST)
        one_hot = (labels[:, None] == ids_blk[None, :]).astype(jnp.float32)
        added = jnp.einsum('ks,sij->kij', one_hot, products, precision=lax.Precision.HIGHEST)
        return running + added, None

    start_sum = jnp.zeros((SN_DEV * N_COL, W, W), jnp.float32)
    contrib, leftover = lax.scan(accumulate, start_sum, (left_all, right_all, slot_ids))
    gram_term = jnp.einsum('kia,kib->kab', diag_inv, diag_inv, precision=lax.Precision.HIGHEST)
    return gram_term - contrib
```

```python
import functools

import jax
import jax.numpy as jnp
from jax import lax
from jax.experimental import pallas as pl
from jax.experimental.pallas import tpu as pltpu
from jax.sharding import PartitionSpec as P

MESH = pl.DeviceIdType.MESH
LANES = 128
ROWS = 16


def split(x):
    hi = x.astype(jnp.bfloat16)
    lo = (x - hi.astype(jnp.float32)).astype(jnp.bfloat16)
    return hi, lo


def transposed_product(a, b):
    ah, al = split(a)
    bh, bl = split(b)
    left = jnp.concatenate([ah, ah, al], axis=0)
    right = jnp.concatenate([bh, bl, bh], axis=0)
    return lax.dot_general(left, right, (((0,), (0,)), ((), ())), preferred_element_type=jnp.float32)


def kernel(
    dims, slots,
    lhat, ainv, dinv, targets, out,
    left, right, fac, ids, prod, rx, last_a, last_b,
    st_y, st_z, rc_y, rc_z, fin_y, fin_z, r2_y, r2_z,
    in_sem, x_send, x_recv, t_send, t_recv,
    ys, yr, zs, zr, y2s, y2r, z2s, z2r,
):
    nx, ny, nz = dims
    row, col = lax.axis_index("row"), lax.axis_index("col")
    y, c = row // 2, row % 2
    x, z = col // nz, col % nz
    none = slots + 1
    half_k = nx * nz // 2
    half_x = nx // 2

    def at(xx, yy, zz, cc):
        return (yy * 2 + cc, xx * nz + zz)

    partner = at(x, y, z, 1 - c)

    def loads(s):
        return (
            pltpu.make_async_copy(lhat.at[s], left.at[s], in_sem.at[0, s]),
            pltpu.make_async_copy(ainv.at[s], right.at[s], in_sem.at[1, s]),
        )

    fac_load = pltpu.make_async_copy(dinv.at[0], fac, in_sem.at[0, slots])
    ids_load = pltpu.make_async_copy(targets, ids, in_sem.at[1, slots])
    fac_load.start()
    ids_load.start()
    for s in range(slots):
        for load in loads(s):
            load.start()

    barrier = pltpu.get_barrier_semaphore()
    peers = [partner]
    for step in (1, ny - 1):
        peers.append(at(x, (y + step) % ny, z, c))
    for step in (1, nz - 1):
        peers.append(at(x, y, (z + step) % nz, c))
    for step in range(1, nx):
        peers.append(at((x + step) % nx, y, z, c))
    for peer in peers:
        pl.semaphore_signal(barrier, inc=1, device_id=peer, device_id_type=MESH)

    prod[none] = jnp.zeros(prod.shape[1:], jnp.float32)
    rx[none] = jnp.zeros(rx.shape[1:], jnp.float32)
    fac_load.wait()
    gram = transposed_product(fac[...], fac[...])
    prod[0] = gram.reshape(prod.shape[1:])
    ids_load.wait()
    pl.semaphore_wait(barrier, len(peers))

    def table(k, carry):
        found = jnp.where(col == k, 0, none)
        for s in range(slots):
            found = jnp.where(ids[s] == k, s + 1, found)
        last_a[k] = found
        return carry

    lax.fori_loop(0, nx * nz, table, 0)
    table_copy = pltpu.make_async_remote_copy(
        last_a, last_b, t_send, t_recv, device_id=partner, device_id_type=MESH
    )
    table_copy.start()

    exchanges = []

    def exchange(s):
        copy = pltpu.make_async_remote_copy(
            prod.at[s, :, 1 - c], rx.at[s], x_send.at[s], x_recv.at[s],
            device_id=partner, device_id_type=MESH,
        )
        copy.start()
        exchanges.append(copy)

    for s in range(slots):
        for load in loads(s):
            load.wait()
        value = transposed_product(left[s], right[s])
        before = jnp.where(ids[s] == col, 0, none)
        for e in range(s):
            before = jnp.where(ids[e] == ids[s], e + 1, before)
        prod[s + 1] = prod[before] - value.reshape(prod.shape[1:])
        exchange(s)
    exchange(slots)
    table_copy.wait()
    for copy in exchanges:
        copy.wait()

    def local_y(k, yb):
        return prod[last_a[k], yb, c, :, 0:LANES] + rx[last_b[k], yb, :, 0:LANES]

    def local_z(k):
        return prod[last_a[k], :, c, :, LANES:] + rx[last_b[k], :, :, LANES:]

    unroll = 4 if half_k % 4 == 0 else 1

    def over_k(body):
        def some(i, carry):
            for j in range(unroll):
                body(i * unroll + j)
            return carry

        lax.fori_loop(0, half_k // unroll, some, 0)

    sends = []

    def hop(axis, way, half, h):
        n = ny if axis == "y" else nz
        long = half == way
        hops = n // 2 if long else n // 2 - 1
        if h >= hops:
            return
        sign = 1 if way == 0 else -1
        first = 0 if long else n // 2
        rc, st, ss, rs = (rc_y, st_y, ys, yr) if axis == "y" else (rc_z, st_z, zs, zr)
        here = y if axis == "y" else z
        dest = (here + sign * (hops - h) + n) % n
        peer = (here + sign + n) % n
        device = at(x, peer, z, c) if axis == "y" else at(x, y, peer, c)
        if h == 0:
            src = st.at[way, half]
        else:
            src = rc.at[way, first + h - 1]
            pltpu.make_async_remote_copy(
                src, src, ss.at[way, first + h - 1], rs.at[way, first + h - 1],
                device_id=device, device_id_type=MESH,
            ).wait_recv()
        if axis == "y":
            def body(k):
                v = local_y(half * half_k + k, dest)
                src[k] = v if h == 0 else src[k] + v

            over_k(body)
        else:
            for i in range(half_x):
                v = local_z((half * half_x + i) * nz + dest)
                src[i] = v if h == 0 else src[i] + v
        copy = pltpu.make_async_remote_copy(
            src, rc.at[way, first + h], ss.at[way, first + h], rs.at[way, first + h],
            device_id=device, device_id_type=MESH,
        )
        copy.start()
        sends.append(copy)

    for h in range(max(ny, nz) // 2):
        for part in (0, 1):
            for axis in ("y", "z"):
                for way in (0, 1):
                    hop(axis, way, way if part == 0 else 1 - way, h)

    def arrived(axis, way, half):
        n = ny if axis == "y" else nz
        long = half == way
        hops = n // 2 if long else n // 2 - 1
        if hops == 0:
            return None
        m = (0 if long else n // 2) + hops - 1
        rc, ss, rs = (rc_y, ys, yr) if axis == "y" else (rc_z, zs, zr)
        pltpu.make_async_remote_copy(
            rc.at[way, m], rc.at[way, m], ss.at[way, m], rs.at[way, m],
            device_id=partner, device_id_type=MESH,
        ).wait_recv()
        return rc.at[way, m]

    for half in (0, 1):
        got_y = [g for g in (arrived("y", way, half) for way in (0, 1)) if g is not None]
        got_z = [g for g in (arrived("z", way, half) for way in (0, 1)) if g is not None]

        def total_y(k):
            v = local_y(half * half_k + k, y)
            for g in got_y:
                v = v + g[k]
            fin_y[half * half_k + k] = v

        over_k(total_y)
        for i in range(half_x):
            xi = half * half_x + i
            v = local_z(xi * nz + z)
            for g in got_z:
                v = v + g[i]
            fin_z[pl.ds(xi * ny, ny)] = v

    n_y, n_z = nx * nz, nx * ny
    place = x * ny + y

    def send_y(d):
        to = (col + d) % n_y
        return pltpu.make_async_remote_copy(
            fin_y.at[to], r2_y.at[col], y2s.at[d], y2r.at[col],
            device_id=(row, to), device_id_type=MESH,
        )

    def send_z(d):
        to = (place + d) % n_z
        return pltpu.make_async_remote_copy(
            fin_z.at[to], r2_z.at[place], z2s.at[d], z2r.at[place],
            device_id=at(to // ny, to % ny, z, c), device_id_type=MESH,
        )

    def start_y(d, carry):
        send_y(d).start()
        return carry

    def start_z(d, carry):
        send_z(d).start()
        return carry

    lax.fori_loop(1, n_y, start_y, 0)
    lax.fori_loop(1, n_z, start_z, 0)

    def take_y(d, total):
        src = (col + d) % n_y
        pltpu.make_async_remote_copy(
            r2_y.at[src], r2_y.at[src], y2s.at[d], y2r.at[src],
            device_id=partner, device_id_type=MESH,
        ).wait_recv()
        return total + r2_y[src]

    def take_z(d, total):
        src = (place + d) % n_z
        pltpu.make_async_remote_copy(
            r2_z.at[src], r2_z.at[src], z2s.at[d], z2r.at[src],
            device_id=partner, device_id_type=MESH,
        ).wait_recv()
        return total + r2_z[src]

    out[0, :, 0:LANES] = lax.fori_loop(1, n_y, take_y, fin_y[col])
    out[0, :, LANES:] = lax.fori_loop(1, n_z, take_z, fin_z[place])

    for copy in sends:
        copy.wait_send()

    def done_y(d, carry):
        send_y(d).wait_send()
        return carry

    def done_z(d, carry):
        send_z(d).wait_send()
        return carry

    lax.fori_loop(1, n_y, done_y, 0)
    lax.fori_loop(1, n_z, done_z, 0)


def on_device(dims, lhat, ainv_anc, diag_inv, targets):
    nx, ny, nz = dims
    slots, height, width = lhat.shape
    f32 = jnp.float32
    vm = pltpu.VMEM
    dma = pltpu.SemaphoreType.DMA
    k_all, half_k, half_x = nx * nz, nx * nz // 2, nx // 2
    scratch = [
        vm((slots, height, width), f32),
        vm((slots, height, width), f32),
        vm((ROWS, width), f32),
        pltpu.SMEM((slots,), jnp.int32),
        vm((slots + 2, ny, 2, ROWS, width), f32),
        vm((slots + 2, ny, ROWS, width), f32),
        pltpu.SMEM((k_all,), jnp.int32),
        pltpu.SMEM((k_all,), jnp.int32),
        vm((2, 2, half_k, ROWS, LANES), f32),
        vm((2, 2, half_x, ny, ROWS, LANES), f32),
        vm((2, ny - 1, half_k, ROWS, LANES), f32),
        vm((2, nz - 1, half_x, ny, ROWS, LANES), f32),
        vm((k_all, ROWS, LANES), f32),
        vm((nx * ny, ROWS, LANES), f32),
        vm((k_all, ROWS, LANES), f32),
        vm((nx * ny, ROWS, LANES), f32),
        dma((2, slots + 1)),
        dma((slots + 1,)),
        dma((slots + 1,)),
        dma,
        dma,
        dma((2, ny - 1)),
        dma((2, ny - 1)),
        dma((2, nz - 1)),
        dma((2, nz - 1)),
        dma((k_all,)),
        dma((k_all,)),
        dma((nx * ny,)),
        dma((nx * ny,)),
    ]
    return pl.pallas_call(
        functools.partial(kernel, dims, slots),
        out_shape=jax.ShapeDtypeStruct(diag_inv.shape, f32),
        in_specs=[pl.BlockSpec(memory_space=pl.ANY)] * 4,
        out_specs=pl.BlockSpec(memory_space=vm),
        scratch_shapes=scratch,
        compiler_params=pltpu.CompilerParams(
            collective_id=0, has_side_effects=True
        ),
        name="selected_blocks",
    )(lhat, ainv_anc, diag_inv, targets.reshape(slots))


def solution(mesh, nz=8):
    dims = (mesh.shape["col"] // nz, mesh.shape["row"] // 2, nz)
    placed = (
        P(("row", "col"), None, None),
        P(("row", "col"), None, None),
        P("col", "row", None),
        P(("row", "col"), None),
    )
    return jax.shard_map(
        functools.partial(on_device, dims), mesh=mesh, in_specs=placed, out_specs=P("col", "row", None), check_vma=False
    )
```

```python
import functools

import jax
import jax.numpy as jnp
from jax import lax
from jax.experimental import pallas as pl
from jax.experimental.pallas import tpu as pltpu
from jax.sharding import PartitionSpec as P

MESH = pl.DeviceIdType.MESH
LANES = 128
SUB = 8


def split(x):
    hi = x.astype(jnp.bfloat16)
    lo = (x - hi.astype(jnp.float32)).astype(jnp.bfloat16)
    return hi, lo


def transposed_product(a, b):
    ah, al = split(a)
    bh, bl = split(b)
    left = jnp.concatenate([ah, ah, al], axis=0)
    right = jnp.concatenate([bh, bl, bh], axis=0)
    return lax.dot_general(left, right, (((0,), (0,)), ((), ())), preferred_element_type=jnp.float32)


def kernel(
    dims, slots,
    lhat, ainv, dinv, targets, out,
    both, fac, ids, prod, rx_u, rx_d, rx_p, last_a, last_o,
    st_uy, st_uz, st_py, st_pz, rc_uy, rc_uz, rc_py, rc_pz,
    fin_uy, fin_uz, fin_py, fin_pz, r2_uy, r2_uz, r2_py, r2_pz,
    in_sem, xu_s, xu_r, xd_s, xd_r, xp_s, xp_r, t_s, t_r,
    uys, uyr, uzs, uzr, ps, pr,
    fus, fuyr, fuzr, fps, fpyr, fpzr,
):
    nx, ny, nz = dims
    row, col = lax.axis_index("row"), lax.axis_index("col")
    y, c = row // 2, row % 2
    x, z = col // nz, col % nz
    h = x % 2
    none = slots + 1
    half_k = nx * nz // 2
    half_x = nx // 2

    def wrap(v, n):
        return jnp.where(v >= n, v - n, v)

    xs = [x] + [wrap(x + d, nx) for d in range(1, nx)]
    yy = [y] + [wrap(y + d, ny) for d in range(1, ny)]
    zz = [z] + [wrap(z + d, nz) for d in range(1, nz)]

    def at(xv, yv, zv, cv):
        return (yv * 2 + cv, xv * nz + zv)

    partner = at(x, y, z, 1 - c)
    pair_y = jnp.where(h == 0, xs[1], xs[nx - 1])
    pair_z = jnp.where(h == 0, xs[nx - 1], xs[1])

    def remote(src, dst, ss, rs, device):
        return pltpu.make_async_remote_copy(src, dst, ss, rs, device_id=device, device_id_type=MESH)

    def loads(s):
        return (
            pltpu.make_async_copy(lhat.at[s], both.at[s, 0], in_sem.at[s]),
            pltpu.make_async_copy(ainv.at[s], both.at[s, 1], in_sem.at[s]),
        )

    fac_load = pltpu.make_async_copy(dinv.at[0], fac, in_sem.at[slots])
    ids_load = pltpu.make_async_copy(targets, ids, in_sem.at[slots + 1])
    ids_load.start()
    fac_load.start()
    for s in range(slots):
        for load in loads(s):
            load.start()

    barrier = pltpu.get_barrier_semaphore()
    peers = [partner, at(x, yy[1], z, c), at(x, yy[ny - 1], z, c), at(x, y, zz[1], c), at(x, y, zz[nz - 1], c)]
    for d in range(1, nx):
        peers += [at(xs[d], y, z, c), at(xs[d], y, z, 1 - c)]
    for peer in peers:
        pl.semaphore_signal(barrier, inc=1, device_id=peer, device_id_type=MESH)

    prod[none] = jnp.zeros(prod.shape[1:], jnp.float32)
    rx_u[none] = jnp.zeros(rx_u.shape[1:], jnp.float32)
    rx_d[none] = jnp.zeros(rx_d.shape[1:], jnp.float32)
    for i in range(2):
        rx_p[i, none] = jnp.zeros(rx_p.shape[2:], jnp.float32)

    def put(s, value, before):
        for i in range(2):
            part = value[:, i * LANES : (i + 1) * LANES].reshape(prod.shape[2:])
            prod[s, i] = part if before is None else prod[before, i] - part

    ids_load.wait()

    def table(k, carry):
        found = jnp.where(col == k, 0, none)
        for s in range(slots):
            found = jnp.where(ids[s] == k, s + 1, found)
        last_a[k] = found
        return carry

    lax.fori_loop(0, nx * nz, table, 0)
    fac_load.wait()
    put(0, transposed_product(fac[...], fac[...]), None)
    pl.semaphore_wait(barrier, len(peers))

    to_py = at(pair_y, y, z, 0)
    to_pz = at(pair_z, y, z, 1)
    tables = [
        remote(last_a, last_o.at[0], t_s, t_r.at[0], partner),
        remote(last_a, last_o.at[1 + c], t_s, t_r.at[1], to_py),
        remote(last_a, last_o.at[1 + c], t_s, t_r.at[1], to_pz),
    ]
    for copy in tables:
        copy.start()

    def exchanges(s):
        return (
            remote(prod.at[s, 0, :, 1 - h, 1], rx_p.at[c, s], xp_s, xp_r, to_py),
            remote(prod.at[s, 1, :, 1 - h, 1], rx_p.at[c, s], xp_s, xp_r, to_pz),
            remote(prod.at[s, :, :, 1 - c, 0], rx_u.at[s], xu_s, xu_r, partner),
            remote(prod.at[s, 1 - c, :, h, 1], rx_d.at[s], xd_s, xd_r, partner),
        )

    for s in range(slots):
        pltpu.make_async_copy(both.at[s], both.at[s], in_sem.at[s]).wait()
        value = transposed_product(both[s, 0], both[s, 1])
        before = jnp.where(ids[s] == col, 0, none)
        for e in range(s):
            before = jnp.where(ids[e] == ids[s], e + 1, before)
        put(s + 1, value, before)
        for copy in exchanges(s):
            copy.start()
    for copy in exchanges(slots):
        copy.start()

    def local_uy(k, yb):
        return prod[last_a[k], 0, yb, c, 0] + rx_u[last_o[0, k], 0, yb]

    def local_uz(k):
        return prod[last_a[k], 1, :, c, 0] + rx_u[last_o[0, k], 1]

    def local_py(k, yb):
        own = prod[last_a[k], 0, yb, h, 1] + rx_d[last_o[0, k], yb]
        return own + (rx_p[0, last_o[1, k], yb] + rx_p[1, last_o[2, k], yb])

    def local_pz(k):
        own = prod[last_a[k], 1, :, h, 1] + rx_d[last_o[0, k]]
        return own + (rx_p[0, last_o[1, k]] + rx_p[1, last_o[2, k]])

    unroll = 4 if half_k % 4 == 0 else 1

    def over_k(body):
        def some(i, carry):
            for j in range(unroll):
                body(i * unroll + j)
            return carry

        lax.fori_loop(0, half_k // unroll, some, 0)

    parts = {
        "uy": (st_uy, rc_uy, uys, uyr, local_uy, ny, yy),
        "uz": (st_uz, rc_uz, uzs, uzr, local_uz, nz, zz),
        "py": (st_py, rc_py, ps, pr, local_py, ny, yy),
        "pz": (st_pz, rc_pz, ps, pr, local_pz, nz, zz),
    }

    def place_of(which, way, half, hop):
        n = parts[which][5]
        hops = n // 2 if half == way else n // 2 - 1
        return hops, (0 if half == way else n // 2) + hop

    def message(which, way, m):
        st, rc, ss, rs, _, n, at_axis = parts[which]
        to = at_axis[1 if way == 0 else n - 1]
        device = at(x, to, z, c) if which[1] == "y" else at(x, y, to, c)
        return remote(st.at[way, m], rc.at[way, m], ss, rs.at[way, m], device)

    def terms(which, half, dest, dst):
        local = parts[which][4]
        if which[1] == "y":
            def body(k):
                dst[k] = local(half * half_k + k, dest)

            over_k(body)
        else:
            for i in range(half_x):
                dst[i] = local((half * half_x + i) * nz + dest)

    def flows(which, hop):
        for late in (0, 1):
            for way in (0, 1):
                half = way if late == 0 else 1 - way
                hops, m = place_of(which, way, half, hop)
                if hop < hops:
                    yield way, half, hops, m

    def prepare(which, hop):
        st, _, _, _, _, n, at_axis = parts[which]
        for way, half, hops, m in flows(which, hop):
            dest = at_axis[(hops - hop) % n if way == 0 else (n - hops + hop) % n]
            terms(which, half, dest, st.at[way, m])

    def go(whiches, hop):
        lists = [[(w, f) for f in flows(w, hop)] for w in whiches]
        for i in range(max(len(found) for found in lists)):
            for found in lists:
                if i >= len(found):
                    continue
                which, (way, half, hops, m) = found[i]
                st, rc = parts[which][0], parts[which][1]
                if hop > 0:
                    message(which, way, m - 1).wait_recv()
                    st[way, m] = st[way, m] + rc[way, m - 1]
                message(which, way, m).start()

    def finish(which, fin):
        _, rc, _, _, _, n, at_axis = parts[which]
        for half in (0, 1):
            for way in (0, 1):
                hops, m = place_of(which, way, half, 0)
                if hops == 0:
                    continue
                m = m + hops - 1
                message(which, way, m).wait_recv()
                fin[half] = fin[half] + rc[way, m]

    def prepare_final(which, fin):
        for half in (0, 1):
            terms(which, half, parts[which][6][0], fin.at[half])

    def for_core(first, second):
        pl.when(c == 0)(first)
        pl.when(c == 1)(second)

    rounds = max(ny, nz) // 2

    def p_round(hop):
        def run(which):
            def body():
                prepare(which, hop)
                go([which], hop)

            return body

        if hop < rounds:
            for_core(run("py"), run("pz"))

    used = pl.ds(0, slots + 1)

    def whole(ref, sem):
        return remote(ref, ref, sem, sem, partner)

    tables[0].wait_recv()
    whole(rx_u.at[used], xu_r).wait_recv()

    def u_round(hop):
        if hop < rounds:
            prepare("uy", hop)
            prepare("uz", hop)
            go(["uy", "uz"], hop)

    u_round(0)
    u_round(1)
    whole(last_o.at[pl.ds(1, 2)], t_r.at[1]).wait_recv()
    whole(rx_d.at[used], xd_r).wait_recv()
    whole(rx_p.at[:, used], xp_r).wait_recv()
    p_round(0)
    u_round(2)
    p_round(1)
    u_round(3)
    p_round(2)
    prepare_final("uy", fin_uy)
    prepare_final("uz", fin_uz)
    finish("uy", fin_uy)
    finish("uz", fin_uz)

    def far(d, n):
        return min(d, n - d)

    xz = sorted(((dx, dz) for dx in range(nx) for dz in range(nz)), key=lambda p: -far(p[0], nx) - far(p[1], nz))
    xy = sorted(((dx, dy) for dx in range(nx) for dy in range(ny)), key=lambda p: -far(p[0], nx) - far(p[1], ny))
    here_z = x * ny + y

    def src_y(fin, dx, dz):
        k = xs[dx] * nz + zz[dz]
        return fin.at[xs[dx] // half_x, k - (xs[dx] // half_x) * half_k]

    def src_z(fin, dx, dy):
        upper = xs[dx] // half_x
        return fin.at[upper, xs[dx] - upper * half_x, yy[dy]]

    def send_uy(dx, dz):
        return remote(
            src_y(fin_uy, dx, dz), r2_uy.at[col], fus.at[0], fuyr, at(xs[dx], y, zz[dz], c)
        )

    def send_uz(dx, dy):
        return remote(
            src_z(fin_uz, dx, dy), r2_uz.at[here_z], fus.at[1], fuzr, at(xs[dx], yy[dy], z, c)
        )

    def send_py(dx, dz):
        return remote(
            src_y(fin_py, dx, dz), r2_py.at[col], fps, fpyr, at(xs[dx], y, zz[dz], h)
        )

    def send_pz(dx, dy):
        return remote(
            src_z(fin_pz, dx, dy), r2_pz.at[here_z], fps, fpzr, at(xs[dx], yy[dy], z, h)
        )

    for i in range(max(len(xz), len(xy))):
        if i < len(xz) and xz[i] != (0, 0):
            send_uy(*xz[i]).start()
        if i < len(xy) and xy[i] != (0, 0):
            send_uz(*xy[i]).start()

    p_round(3)

    def p_final(which, fin, pairs, send, keep):
        def body():
            prepare_final(which, fin)
            finish(which, fin)
            for pair in pairs:
                if pair == (0, 0):
                    pl.when(h == c)(keep)
                    pl.when(h != c)(lambda: send(0, 0).start())
                else:
                    send(*pair).start()

        return body

    def keep_y():
        r2_py[col] = src_y(fin_py, 0, 0)[...]

    def keep_z():
        r2_pz[here_z] = src_z(fin_pz, 0, 0)[...]

    for_core(
        p_final("py", fin_py, xz, send_py, keep_y),
        p_final("pz", fin_pz, xy, send_pz, keep_z),
    )

    whole(last_o, t_s).wait_send()
    whole(rx_u.at[used], xu_s).wait_send()
    whole(rx_d.at[used], xd_s).wait_send()
    whole(rx_p.at[:, used], xp_s).wait_send()
    whole(st_uy, uys).wait_send()
    whole(st_uz, uzs).wait_send()
    for_core(lambda: whole(st_py, ps).wait_send(), lambda: whole(st_pz, ps).wait_send())

    def collect(r2, skip, first):
        total = first
        for k in range(r2.shape[0]):
            total = total + jnp.where(skip == k, 0.0, r2[k])
        return total

    n_y, n_z = nx * nz, nx * ny
    whole(r2_uy.at[pl.ds(0, n_y - 1)], fuyr).wait_recv()
    out[0, 0:SUB, 0:LANES] = collect(r2_uy, col, src_y(fin_uy, 0, 0)[...])
    whole(r2_uz.at[pl.ds(0, n_z - 1)], fuzr).wait_recv()
    out[0, 0:SUB, LANES:] = collect(r2_uz, here_z, src_z(fin_uz, 0, 0)[...])

    def collect_p(r2, sem, n, own_core):
        mine = (h == c) & (c == own_core)
        pl.when(mine)(lambda: whole(r2.at[pl.ds(0, half_x * n - 1)], sem).wait_recv())
        pl.when(jnp.logical_not(mine))(lambda: whole(r2.at[pl.ds(0, half_x * n)], sem).wait_recv())
        total = None
        for i in range(half_x):
            for d in range(n):
                value = r2[(2 * i + c) * n + d]
                total = value if total is None else total + value
        return total

    out[0, SUB:, 0:LANES] = collect_p(r2_py, fpyr, nz, 0)
    out[0, SUB:, LANES:] = collect_p(r2_pz, fpzr, ny, 1)

    whole(r2_uy.at[pl.ds(0, n_y - 1)], fus.at[0]).wait_send()
    whole(r2_uz.at[pl.ds(0, n_z - 1)], fus.at[1]).wait_send()

    def p_sent(n):
        pl.when(h == c)(lambda: whole(r2_py.at[pl.ds(0, n - 1)], fps).wait_send())
        pl.when(h != c)(lambda: whole(r2_py.at[pl.ds(0, n)], fps).wait_send())

    for_core(lambda: p_sent(n_y), lambda: p_sent(n_z))


def on_device(dims, lhat, ainv_anc, diag_inv, targets):
    nx, ny, nz = dims
    slots, height, width = lhat.shape
    f32 = jnp.float32
    dma = pltpu.SemaphoreType.DMA
    k_all, half_k, half_x = nx * nz, nx * nz // 2, nx // 2
    tile = (SUB, LANES)

    def vm(*lead):
        return pltpu.VMEM((*lead, *tile), f32)

    stages_y = [vm(2, ny - 1, half_k)]
    stages_z = [vm(2, nz - 1, half_x, ny)]
    scratch = [
        pltpu.VMEM((slots, 2, height, width), f32),
        pltpu.VMEM(diag_inv.shape[1:], f32),
        pltpu.SMEM((slots,), jnp.int32),
        vm(slots + 2, 2, ny, 2, 2),
        vm(slots + 2, 2, ny),
        vm(slots + 2, ny),
        vm(2, slots + 2, ny),
        pltpu.SMEM((k_all,), jnp.int32),
        pltpu.SMEM((3, k_all), jnp.int32),
        *(stages_y + stages_z) * 4,
        *[vm(2, half_k), vm(2, half_x, ny)] * 2,
        *[vm(k_all), vm(nx * ny)] * 2,
        dma((slots + 2,)),
        *[dma] * 6,
        dma,
        dma((2,)),
        dma,
        dma((2, ny - 1)),
        dma,
        dma((2, nz - 1)),
        dma,
        dma((2, max(ny, nz) - 1)),
        dma((2,)),
        *[dma] * 5,
    ]
    return pl.pallas_call(
        functools.partial(kernel, dims, slots),
        out_shape=jax.ShapeDtypeStruct(diag_inv.shape, f32),
        in_specs=[pl.BlockSpec(memory_space=pltpu.HBM)] * 4,
        out_specs=pl.BlockSpec(memory_space=pltpu.VMEM),
        scratch_shapes=scratch,
        compiler_params=pltpu.CompilerParams(
            collective_id=0, has_side_effects=True
        ),
        name="selected_blocks",
    )(lhat, ainv_anc, diag_inv, targets.reshape(slots))


def solution(mesh, nz=8):
    dims = (mesh.shape["col"] // nz, mesh.shape["row"] // 2, nz)
    placed = (
        P(("row", "col"), None, None),
        P(("row", "col"), None, None),
        P("col", "row", None),
        P(("row", "col"), None),
    )
    return jax.shard_map(
        functools.partial(on_device, dims), mesh=mesh, in_specs=placed, out_specs=P("col", "row", None), check_vma=False
    )
```

```python
import functools

import jax
import jax.numpy as jnp
from jax import lax
from jax.experimental import pallas as pl
from jax.experimental.pallas import tpu as pltpu
from jax.sharding import PartitionSpec as P

MESH = pl.DeviceIdType.MESH
LANES = 128
SUB = 8
U, V = 1, 0


def split(x):
    hi = x.astype(jnp.bfloat16)
    lo = (x - hi.astype(jnp.float32)).astype(jnp.bfloat16)
    return hi, lo


def transposed_product(a, b):
    ah, al = split(a)
    bh, bl = split(b)
    left = jnp.concatenate([ah, ah, al], axis=0)
    right = jnp.concatenate([bh, bl, bh], axis=0)
    return lax.dot_general(left, right, (((0,), (0,)), ((), ())), preferred_element_type=jnp.float32)


def kernel(
    dims, slots,
    lhat, ainv, dinv, targets, out,
    both, fac, ids, prod, rx_u, rx_d, rx_p, last_a, last_o,
    st_uy, st_uz, st_py, st_pz, rc_uy, rc_uz, rc_py, rc_pz,
    fin_uy, fin_uz, fin_py, fin_pz, r2_uy, r2_uz, r2_py, r2_pz,
    in_sem, d_s, d_r, xp_s, xp_r, t_s, t_r,
    ys, yr, zs, zr, fs, fuyr, fuzr, fpyr, fpzr,
):
    nx, ny, nz = dims
    row, col = lax.axis_index("row"), lax.axis_index("col")
    y, c = row // 2, row % 2
    x, z = col // nz, col % nz
    h = x % 2
    none = slots + 1
    half_x = nx // 2

    def wrap(v, n):
        return jnp.where(v >= n, v - n, v)

    xs = [x] + [wrap(x + d, nx) for d in range(1, nx)]
    yy = [y] + [wrap(y + d, ny) for d in range(1, ny)]
    zz = [z] + [wrap(z + d, nz) for d in range(1, nz)]

    def at(xv, yv, zv, cv):
        return (yv * 2 + cv, xv * nz + zv)

    partner = at(x, y, z, 1 - c)
    pair_y = jnp.where(h == 0, xs[1], xs[nx - 1])
    pair_z = jnp.where(h == 0, xs[nx - 1], xs[1])

    def remote(src, dst, ss, rs, device):
        return pltpu.make_async_remote_copy(src, dst, ss, rs, device_id=device, device_id_type=MESH)

    def loads(s):
        return (
            pltpu.make_async_copy(lhat.at[s], both.at[s, 0], in_sem.at[s]),
            pltpu.make_async_copy(ainv.at[s], both.at[s, 1], in_sem.at[s]),
        )

    fac_load = pltpu.make_async_copy(dinv.at[0], fac, in_sem.at[slots])
    ids_load = pltpu.make_async_copy(targets, ids, in_sem.at[slots + 1])
    ids_load.start()
    fac_load.start()
    for s in range(slots):
        for load in loads(s):
            load.start()

    barrier = pltpu.get_barrier_semaphore()
    peers = [partner, at(x, yy[1], z, c), at(x, yy[ny - 1], z, c), at(x, y, zz[1], c), at(x, y, zz[nz - 1], c)]
    for d in range(1, nx):
        peers += [at(xs[d], y, z, c), at(xs[d], y, z, 1 - c)]
    if (nx, ny, nz) == (4, 8, 8):
        for d in (2, 6):
            peers += [at(x, yy[d], z, c), at(x, y, zz[d], c)]
    for peer in peers:
        pl.semaphore_signal(barrier, inc=1, device_id=peer, device_id_type=MESH)

    prod[none] = jnp.zeros(prod.shape[1:], jnp.float32)
    rx_u[none] = jnp.zeros(rx_u.shape[1:], jnp.float32)
    rx_d[none] = jnp.zeros(rx_d.shape[1:], jnp.float32)
    for i in range(2):
        for j in range(2):
            rx_p[i, j, none] = jnp.zeros(rx_p.shape[3:], jnp.float32)

    def put(s, value, before):
        for i in range(2):
            part = value[:, i * LANES : (i + 1) * LANES].reshape(prod.shape[2:])
            prod[s, i] = part if before is None else prod[before, i] - part

    ids_load.wait()

    def table(k, carry):
        found = jnp.where(col == k, 0, none)
        for s in range(slots):
            found = jnp.where(ids[s] == k, s + 1, found)
        last_a[k] = found
        return carry

    lax.fori_loop(0, nx * nz, table, 0)
    fac_load.wait()
    put(0, transposed_product(fac[...], fac[...]), None)
    pl.semaphore_wait(barrier, len(peers))

    to_py = at(pair_y, y, z, V)
    to_pz = at(pair_z, y, z, V)
    tables = [
        remote(last_a, last_o.at[0], t_s, t_r.at[0], partner),
        remote(last_a, last_o.at[1 + c], t_s, t_r.at[1], to_py),
        remote(last_a, last_o.at[3 + c], t_s, t_r.at[1], to_pz),
    ]
    for copy in tables:
        copy.start()

    def across(s):
        return (
            remote(prod.at[s, 0, :, 1 - h, 1], rx_p.at[0, c, s], xp_s, xp_r, to_py),
            remote(prod.at[s, 1, :, 1 - h, 1], rx_p.at[1, c, s], xp_s, xp_r, to_pz),
        )

    def exchange(s):
        for copy in across(s):
            copy.start()

        @pl.when(c == U)
        def _():
            remote(prod.at[s, :, :, h, 1], rx_d.at[s], d_s, d_r, partner).start()

        @pl.when(c == V)
        def _():
            remote(prod.at[s, :, :, :, 0], rx_u.at[s], d_s, d_r, partner).start()

    for s in range(slots):
        pltpu.make_async_copy(both.at[s], both.at[s], in_sem.at[s]).wait()
        value = transposed_product(both[s, 0], both[s, 1])
        before = jnp.where(ids[s] == col, 0, none)
        for e in range(s):
            before = jnp.where(ids[e] == ids[s], e + 1, before)
        put(s + 1, value, before)
        exchange(s)
    exchange(slots)

    def local_uy(k, yb):
        return prod[last_a[k], 0, yb, :, 0] + rx_u[last_o[0, k], 0, yb]

    def local_uz(k):
        return prod[last_a[k], 1, :, :, 0] + rx_u[last_o[0, k], 1]

    def local_py(k, yb):
        own = prod[last_a[k], 0, yb, h, 1] + rx_d[last_o[0, k], 0, yb]
        return own + (rx_p[0, 0, last_o[1, k], yb] + rx_p[0, 1, last_o[2, k], yb])

    def local_pz(k):
        own = prod[last_a[k], 1, :, h, 1] + rx_d[last_o[0, k], 1]
        return own + (rx_p[1, 0, last_o[3, k]] + rx_p[1, 1, last_o[4, k]])

    parts = {
        "uy": (st_uy, rc_uy, ys, yr, local_uy, ny, yy),
        "uz": (st_uz, rc_uz, zs, zr, local_uz, nz, zz),
        "py": (st_py, rc_py, ys, yr, local_py, ny, yy),
        "pz": (st_pz, rc_pz, zs, zr, local_pz, nz, zz),
    }

    def place_of(which, way, q, hop):
        n = parts[which][5]
        long = (q < half_x) == (way == 0)
        hops = n // 2 if long else n // 2 - 1
        base = (q % half_x) * hops + (0 if long else half_x * (n // 2))
        return hops, base + hop

    def message(which, way, m):
        st, rc, ss, rs, _, n, at_axis = parts[which]
        to = at_axis[1 if way == 0 else n - 1]
        device = at(x, to, z, c) if which[1] == "y" else at(x, y, to, c)
        return remote(st.at[way, m], rc.at[way, m], ss, rs.at[way, m], device)

    def terms(which, q, dest, dst):
        local = parts[which][4]
        if which[1] == "y":
            for i in range(nz):
                dst[i] = local(q * nz + i, dest)
        else:
            dst[...] = local(q * nz + dest)

    def flows(which, hop):
        for late in (0, 1):
            for j in range(half_x):
                for way in (0, 1):
                    q = (way if late == 0 else 1 - way) * half_x + j
                    hops, m = place_of(which, way, q, hop)
                    if hop < hops:
                        yield way, q, hops, m

    def own(which, hop, way, q, hops, m):
        st, _, _, _, _, n, at_axis = parts[which]
        dest = at_axis[(hops - hop) % n if way == 0 else (n - hops + hop) % n]
        terms(which, q, dest, st.at[way, m])

    def prepare(which, hop):
        for flow in flows(which, hop):
            own(which, hop, *flow)

    def go(whiches, hop):
        lists = [[(w, f) for f in flows(w, hop)] for w in whiches]
        for i in range(max(len(found) for found in lists)):
            for found in lists:
                if i >= len(found):
                    continue
                which, (way, q, hops, m) = found[i]
                st, rc = parts[which][0], parts[which][1]
                if hop == 0:
                    own(which, hop, way, q, hops, m)
                else:
                    message(which, way, m - 1).wait_recv()
                    st[way, m] = st[way, m] + rc[way, m - 1]
                message(which, way, m).start()

    def finish(which, fin):
        _, rc, _, _, _, n, at_axis = parts[which]
        for q in range(nx):
            for way in (0, 1):
                hops, m = place_of(which, way, q, 0)
                if hops == 0:
                    continue
                m = m + hops - 1
                message(which, way, m).wait_recv()
                fin[q] = fin[q] + rc[way, m]

    def prepare_final(which, fin):
        for q in range(nx):
            terms(which, q, parts[which][6][0], fin.at[q])

    def hop_message(which, way, m, steps):
        st, rc, ss, rs, _, n, at_axis = parts[which]
        to = at_axis[steps if way == 0 else n - steps]
        device = at(x, to, z, c) if which[1] == "y" else at(x, y, to, c)
        return remote(st.at[way, m], rc.at[way, m], ss, rs.at[way, m], device)

    def strides(pair, fins):
        def term(which, way, m, q, steps):
            n, at_axis = parts[which][5:]
            terms(which, q, at_axis[steps if way == 0 else n - steps], parts[which][0].at[way, m])

        everything = [(which, way) for which in pair for way in (0, 1)]
        for j in range(2):
            for which, way in everything:
                term(which, way, 4 + j, way * 2 + j, 4)
                hop_message(which, way, 4 + j, 2).start()
        for q in (0, 2, 1, 3):
            for which, way in everything:
                term(which, way, q, q, 3)
                hop_message(which, way, q, 1).start()
        for q in range(4):
            for which, way in everything:
                term(which, way, 6 + q, q, 1)
        for q in range(4):
            for which, way in everything:
                term(which, way, 10 + q, q, 2)
        for which, fin in zip(pair, fins):
            prepare_final(which, fin)
        for q in (0, 2, 1, 3):
            for which, way in everything:
                st, rc = parts[which][:2]
                value = st[way, 10 + q]
                if q // 2 == way:
                    hop_message(which, way, 4 + q % 2, 2).wait_recv()
                    value = value + rc[way, 4 + q % 2]
                hop_message(which, way, q, 1).wait_recv()
                st[way, 10 + q] = value + rc[way, q]
                hop_message(which, way, 10 + q, 2).start()
        for q in range(4):
            for which, way in everything:
                hop_message(which, way, 6 + q, 1).start()
        for m, steps in ((6, 1), (10, 2)):
            for q in (0, 2, 1, 3):
                for which, fin in zip(pair, fins):
                    for way in (0, 1):
                        hop_message(which, way, m + q, steps).wait_recv()
                        fin[q] = fin[q] + parts[which][1][way, m + q]

    used = pl.ds(0, slots + 1)

    def whole(ref, sem):
        return remote(ref, ref, sem, sem, partner)

    tables[0].wait_recv()

    def far(d, n):
        return min(d, n - d)

    xz = sorted(((dx, dz) for dx in range(nx) for dz in range(nz)), key=lambda p: -far(p[0], nx) - far(p[1], nz))
    xy = sorted(((dx, dy) for dx in range(nx) for dy in range(ny)), key=lambda p: -far(p[0], nx) - far(p[1], ny))
    here_z = x * ny + y

    def src_y(fin, dx, dz):
        return fin.at[xs[dx], zz[dz]]

    def src_z(fin, dx, dy):
        return fin.at[xs[dx], yy[dy]]

    n_y, n_z = nx * nz, nx * ny

    def send_u(dx, d, to):
        return (
            remote(src_y(fin_uy, dx, d).at[to], r2_uy.at[col], fs.at[0], fuyr, at(xs[dx], y, zz[d], to)),
            remote(src_z(fin_uz, dx, d).at[to], r2_uz.at[here_z], fs.at[1], fuzr, at(xs[dx], yy[d], z, to)),
        )

    def send_p(dx, d):
        return (
            remote(src_y(fin_py, dx, d), r2_py.at[col], fs.at[0], fpyr, at(xs[dx], y, zz[d], h)),
            remote(src_z(fin_pz, dx, d), r2_pz.at[here_z], fs.at[1], fpzr, at(xs[dx], yy[d], z, h)),
        )

    def chains(first, second, fin_first, fin_second):
        for hop in range(max(ny, nz) // 2):
            if hop > 0:
                prepare(first, hop)
                prepare(second, hop)
            go([first, second], hop)
        prepare_final(first, fin_first)
        prepare_final(second, fin_second)
        finish(first, fin_first)
        finish(second, fin_second)

    def each(body):
        for i in range(max(len(xz), len(xy))):
            for which, pairs in enumerate((xz, xy)):
                if i < len(pairs):
                    body(which, *pairs[i])

    @pl.when(c == U)
    def _():
        whole(rx_u.at[used], d_r).wait_recv()
        chains("uy", "uz", fin_uy, fin_uz)

        def send(which, dx, d):
            for to in (V, U):
                if (dx, d, to) != (0, 0, U):
                    send_u(dx, d, to)[which].start()

        each(send)
        r2_uy[col] = src_y(fin_uy, 0, 0)[U]
        r2_uz[here_z] = src_z(fin_uz, 0, 0)[U]
        whole(rx_d.at[used], d_s).wait_send()
        whole(st_uy, ys).wait_send()
        whole(st_uz, zs).wait_send()

    @pl.when(c == V)
    def _():
        whole(last_o.at[pl.ds(1, 4)], t_r.at[1]).wait_recv()
        whole(rx_d.at[used], d_r).wait_recv()
        whole(rx_p.at[:, :, used], xp_r).wait_recv()
        if (nx, ny, nz) == (4, 8, 8):
            strides(("py", "pz"), (fin_py, fin_pz))
        else:
            chains("py", "pz", fin_py, fin_pz)

        def send(which, dx, d):
            if (dx, d) != (0, 0):
                send_p(dx, d)[which].start()

        each(send)

        @pl.when(h != V)
        def _():
            for copy in send_p(0, 0):
                copy.start()

        @pl.when(h == V)
        def _():
            r2_py[col] = src_y(fin_py, 0, 0)[...]
            r2_pz[here_z] = src_z(fin_pz, 0, 0)[...]

        whole(rx_u.at[used], d_s).wait_send()
        whole(st_py, ys).wait_send()
        whole(st_pz, zs).wait_send()

    whole(last_o.at[pl.ds(0, 3)], t_s).wait_send()
    whole(rx_p.at[0, :, used], xp_s).wait_send()

    finals = ((r2_uy, n_y, fs.at[0]), (r2_uz, n_z, fs.at[1]))

    def take(r2, sem, count, kept):
        pl.when(kept)(lambda: whole(r2.at[pl.ds(0, count - 1)], sem).wait_recv())
        pl.when(jnp.logical_not(kept))(lambda: whole(r2.at[pl.ds(0, count)], sem).wait_recv())

    def summed(values):
        values = list(values)
        while len(values) > 1:
            values = [a + b for a, b in zip(values[::2], values[1::2])] + values[len(values) // 2 * 2 :]
        return values[0]

    take(r2_uy, fuyr, n_y, c == U)
    out[0, 0:SUB, 0:LANES] = summed(r2_uy[k] for k in range(n_y))
    take(r2_uz, fuzr, n_z, c == U)
    out[0, 0:SUB, LANES:] = summed(r2_uz[k] for k in range(n_z))
    mine = (c == V) & (h == V)
    take(r2_py, fpyr, n_y // 2, mine)
    out[0, SUB:, 0:LANES] = summed(r2_py[(2 * i + c) * nz + d] for i in range(half_x) for d in range(nz))
    take(r2_pz, fpzr, n_z // 2, mine)
    out[0, SUB:, LANES:] = summed(r2_pz[(2 * i + c) * ny + d] for i in range(half_x) for d in range(ny))

    @pl.when(c == U)
    def _():
        for r2, n, sem in finals:
            whole(r2, sem).wait_send()
            whole(r2.at[pl.ds(0, n - 1)], sem).wait_send()

    @pl.when(c == V)
    def _():
        for r2, n, sem in finals:
            whole(r2.at[pl.ds(0, n - 1)], sem).wait_send()
            pl.when(h != V)(lambda: whole(r2.at[0], sem).wait_send())


def on_device(dims, lhat, ainv_anc, diag_inv, targets):
    nx, ny, nz = dims
    slots, height, width = lhat.shape
    f32 = jnp.float32
    dma = pltpu.SemaphoreType.DMA
    k_all = nx * nz
    my, mz = nx // 2 * (ny - 1), nx // 2 * (nz - 1)
    tile = (SUB, LANES)

    def vm(*lead):
        return pltpu.VMEM((*lead, *tile), f32)

    scratch = [
        pltpu.VMEM((slots, 2, height, width), f32),
        pltpu.VMEM(diag_inv.shape[1:], f32),
        pltpu.SMEM((slots,), jnp.int32),
        vm(slots + 2, 2, ny, 2, 2),
        vm(slots + 2, 2, ny, 2),
        vm(slots + 2, 2, ny),
        vm(2, 2, slots + 2, ny),
        pltpu.SMEM((k_all,), jnp.int32),
        pltpu.SMEM((5, k_all), jnp.int32),
        *[vm(2, my, nz, 2), vm(2, mz, ny, 2), vm(2, my, nz), vm(2, mz, ny)] * 2,
        *[vm(nx, nz, 2), vm(nx, ny, 2), vm(nx, nz), vm(nx, ny)],
        *[vm(k_all), vm(nx * ny)] * 2,
        dma((slots + 2,)),
        *[dma] * 5,
        dma((2,)),
        dma,
        dma((2, my)),
        dma,
        dma((2, mz)),
        dma((2,)),
        *[dma] * 4,
    ]
    return pl.pallas_call(
        functools.partial(kernel, dims, slots),
        out_shape=jax.ShapeDtypeStruct(diag_inv.shape, f32),
        in_specs=[pl.BlockSpec(memory_space=pltpu.HBM)] * 4,
        out_specs=pl.BlockSpec(memory_space=pltpu.VMEM),
        scratch_shapes=scratch,
        compiler_params=pltpu.CompilerParams(
            collective_id=0, has_side_effects=True
        ),
        name="selected_blocks",
    )(lhat, ainv_anc, diag_inv, targets.reshape(slots))


def solution(mesh, nz=8):
    dims = (mesh.shape["col"] // nz, mesh.shape["row"] // 2, nz)
    placed = (
        P(("row", "col"), None, None),
        P(("row", "col"), None, None),
        P("col", "row", None),
        P(("row", "col"), None),
    )
    return jax.shard_map(
        functools.partial(on_device, dims), mesh=mesh, in_specs=placed, out_specs=P("col", "row", None), check_vma=False
    )
```

```python
import functools

import jax
import jax.numpy as jnp
from jax import lax
from jax.experimental import pallas as pl
from jax.experimental.pallas import tpu as pltpu
from jax.sharding import PartitionSpec as P

MESH = pl.DeviceIdType.MESH
LANES = 128
SUB = 8
U, V = 0, 1


def split(x):
    hi = x.astype(jnp.bfloat16)
    lo = (x - hi.astype(jnp.float32)).astype(jnp.bfloat16)
    return hi, lo


def transposed_product(a, b):
    ah, al = split(a)
    bh, bl = split(b)
    left = jnp.concatenate([ah, ah, al], axis=0)
    right = jnp.concatenate([bh, bl, bh], axis=0)
    return lax.dot_general(left, right, (((0,), (0,)), ((), ())), preferred_element_type=jnp.float32)


def kernel(
    dims, slots,
    lhat, ainv, dinv, targets, out,
    both, fac, ids, prod, rx_u, rx_d, rx_p, last_a, last_o,
    st_uy, st_uz, st_py, st_pz, rc_uy, rc_uz, rc_py, rc_pz,
    fin_uy, fin_uz, fin_py, fin_pz, r2_uy, r2_uz, r2_py, r2_pz,
    in_sem, d_s, d_r, xp_s, xp_r, t_s, t_r,
    ys, yr, zs, zr, fs, fuyr, fuzr, fpyr, fpzr,
):
    nx, ny, nz = dims
    row, col = lax.axis_index("row"), lax.axis_index("col")
    y, c = row // 2, row % 2
    x, z = col // nz, col % nz
    h = x % 2
    none = slots + 1
    half_x = nx // 2

    def wrap(v, n):
        return jnp.where(v >= n, v - n, v)

    xs = [x] + [wrap(x + d, nx) for d in range(1, nx)]
    yy = [y] + [wrap(y + d, ny) for d in range(1, ny)]
    zz = [z] + [wrap(z + d, nz) for d in range(1, nz)]

    def at(xv, yv, zv, cv):
        return (yv * 2 + cv, xv * nz + zv)

    partner = at(x, y, z, 1 - c)
    pair_y = jnp.where(h == 0, xs[1], xs[nx - 1])
    pair_z = jnp.where(h == 0, xs[nx - 1], xs[1])

    def remote(src, dst, ss, rs, device):
        return pltpu.make_async_remote_copy(src, dst, ss, rs, device_id=device, device_id_type=MESH)

    def loads(s):
        return (
            pltpu.make_async_copy(lhat.at[s], both.at[s, 0], in_sem.at[s]),
            pltpu.make_async_copy(ainv.at[s], both.at[s, 1], in_sem.at[s]),
        )

    fac_load = pltpu.make_async_copy(dinv.at[0], fac, in_sem.at[slots])
    ids_load = pltpu.make_async_copy(targets, ids, in_sem.at[slots + 1])
    ids_load.start()
    fac_load.start()
    for s in range(slots):
        for load in loads(s):
            load.start()

    barrier = pltpu.get_barrier_semaphore()
    peers = [partner, at(x, yy[1], z, c), at(x, yy[ny - 1], z, c), at(x, y, zz[1], c), at(x, y, zz[nz - 1], c)]
    for d in range(1, nx):
        peers += [at(xs[d], y, z, c), at(xs[d], y, z, 1 - c)]
    for peer in peers:
        pl.semaphore_signal(barrier, inc=1, device_id=peer, device_id_type=MESH)

    prod[none] = jnp.zeros(prod.shape[1:], jnp.float32)
    rx_u[none] = jnp.zeros(rx_u.shape[1:], jnp.float32)
    rx_d[none] = jnp.zeros(rx_d.shape[1:], jnp.float32)
    for i in range(2):
        for j in range(2):
            rx_p[i, j, none] = jnp.zeros(rx_p.shape[3:], jnp.float32)

    def put(s, value, before):
        for i in range(2):
            part = value[:, i * LANES : (i + 1) * LANES].reshape(prod.shape[2:])
            prod[s, i] = part if before is None else prod[before, i] - part

    ids_load.wait()

    def table(k, carry):
        found = jnp.where(col == k, 0, none)
        for s in range(slots):
            found = jnp.where(ids[s] == k, s + 1, found)
        last_a[k] = found
        return carry

    lax.fori_loop(0, nx * nz, table, 0)
    fac_load.wait()
    put(0, transposed_product(fac[...], fac[...]), None)
    pl.semaphore_wait(barrier, len(peers))

    to_py = at(pair_y, y, z, V)
    to_pz = at(pair_z, y, z, V)
    tables = [
        remote(last_a, last_o.at[0], t_s, t_r.at[0], partner),
        remote(last_a, last_o.at[1 + c], t_s, t_r.at[1], to_py),
        remote(last_a, last_o.at[3 + c], t_s, t_r.at[1], to_pz),
    ]
    for copy in tables:
        copy.start()

    def across(s):
        return (
            remote(prod.at[s, 0, :, 1 - h, 1], rx_p.at[0, c, s], xp_s, xp_r, to_py),
            remote(prod.at[s, 1, :, 1 - h, 1], rx_p.at[1, c, s], xp_s, xp_r, to_pz),
        )

    def exchange(s):
        @pl.when(c == U)
        def _():
            remote(prod.at[s, :, :, h, 1], rx_d.at[s], d_s, d_r, partner).start()

        @pl.when(c == V)
        def _():
            remote(prod.at[s, :, :, :, 0], rx_u.at[s], d_s, d_r, partner).start()

        for copy in across(s):
            copy.start()

    for s in range(slots):
        pltpu.make_async_copy(both.at[s], both.at[s], in_sem.at[s]).wait()
        value = transposed_product(both[s, 0], both[s, 1])
        before = jnp.where(ids[s] == col, 0, none)
        for e in range(s):
            before = jnp.where(ids[e] == ids[s], e + 1, before)
        put(s + 1, value, before)
        exchange(s)
    exchange(slots)

    def local_uy(k, yb):
        return prod[last_a[k], 0, yb, :, 0] + rx_u[last_o[0, k], 0, yb]

    def local_uz(k):
        return prod[last_a[k], 1, :, :, 0] + rx_u[last_o[0, k], 1]

    def local_py(k, yb):
        own = prod[last_a[k], 0, yb, h, 1] + rx_d[last_o[0, k], 0, yb]
        return own + (rx_p[0, 0, last_o[1, k], yb] + rx_p[0, 1, last_o[2, k], yb])

    def local_pz(k):
        own = prod[last_a[k], 1, :, h, 1] + rx_d[last_o[0, k], 1]
        return own + (rx_p[1, 0, last_o[3, k]] + rx_p[1, 1, last_o[4, k]])

    parts = {
        "uy": (st_uy, rc_uy, ys, yr, local_uy, ny, yy),
        "uz": (st_uz, rc_uz, zs, zr, local_uz, nz, zz),
        "py": (st_py, rc_py, ys, yr, local_py, ny, yy),
        "pz": (st_pz, rc_pz, zs, zr, local_pz, nz, zz),
    }

    def place_of(which, way, q, hop):
        n = parts[which][5]
        long = (q < half_x) == (way == 0)
        hops = n // 2 if long else n // 2 - 1
        base = (q % half_x) * hops + (0 if long else half_x * (n // 2))
        return hops, base + hop

    def message(which, way, m):
        st, rc, ss, rs, _, n, at_axis = parts[which]
        to = at_axis[1 if way == 0 else n - 1]
        device = at(x, to, z, c) if which[1] == "y" else at(x, y, to, c)
        return remote(st.at[way, m], rc.at[way, m], ss, rs.at[way, m], device)

    def terms(which, q, dest, dst):
        local = parts[which][4]
        if which[1] == "y":
            for i in range(nz):
                dst[i] = local(q * nz + i, dest)
        else:
            dst[...] = local(q * nz + dest)

    def flows(which, hop):
        for late in (0, 1):
            for j in range(half_x):
                for way in (0, 1):
                    q = (way if late == 0 else 1 - way) * half_x + j
                    hops, m = place_of(which, way, q, hop)
                    if hop < hops:
                        yield way, q, hops, m

    def own(which, hop, way, q, hops, m):
        st, _, _, _, _, n, at_axis = parts[which]
        dest = at_axis[(hops - hop) % n if way == 0 else (n - hops + hop) % n]
        terms(which, q, dest, st.at[way, m])

    def prepare(which, hop):
        for flow in flows(which, hop):
            own(which, hop, *flow)

    def go(whiches, hop):
        lists = [[(w, f) for f in flows(w, hop)] for w in whiches]
        for i in range(max(len(found) for found in lists)):
            for found in lists:
                if i >= len(found):
                    continue
                which, (way, q, hops, m) = found[i]
                st, rc = parts[which][0], parts[which][1]
                if hop == 0:
                    own(which, hop, way, q, hops, m)
                else:
                    message(which, way, m - 1).wait_recv()
                    st[way, m] = st[way, m] + rc[way, m - 1]
                message(which, way, m).start()

    def finish(which, fin):
        _, rc, _, _, _, n, at_axis = parts[which]
        for q in range(nx):
            for way in (0, 1):
                hops, m = place_of(which, way, q, 0)
                if hops == 0:
                    continue
                m = m + hops - 1
                message(which, way, m).wait_recv()
                fin[q] = fin[q] + rc[way, m]

    def prepare_final(which, fin):
        for q in range(nx):
            terms(which, q, parts[which][6][0], fin.at[q])

    used = pl.ds(0, slots + 1)

    def whole(ref, sem):
        return remote(ref, ref, sem, sem, partner)

    tables[0].wait_recv()

    def far(d, n):
        return min(d, n - d)

    xz = sorted(((dx, dz) for dx in range(nx) for dz in range(nz)), key=lambda p: -far(p[0], nx) - far(p[1], nz))
    xy = sorted(((dx, dy) for dx in range(nx) for dy in range(ny)), key=lambda p: -far(p[0], nx) - far(p[1], ny))
    here_z = x * ny + y

    def src_y(fin, dx, dz):
        return fin.at[xs[dx], zz[dz]]

    def src_z(fin, dx, dy):
        return fin.at[xs[dx], yy[dy]]

    n_y, n_z = nx * nz, nx * ny

    def send_u(dx, d, to):
        return (
            remote(src_y(fin_uy, dx, d).at[to], r2_uy.at[col], fs.at[0], fuyr, at(xs[dx], y, zz[d], to)),
            remote(src_z(fin_uz, dx, d).at[to], r2_uz.at[here_z], fs.at[1], fuzr, at(xs[dx], yy[d], z, to)),
        )

    def send_p(dx, d):
        return (
            remote(src_y(fin_py, dx, d), r2_py.at[col], fs.at[0], fpyr, at(xs[dx], y, zz[d], h)),
            remote(src_z(fin_pz, dx, d), r2_pz.at[here_z], fs.at[1], fpzr, at(xs[dx], yy[d], z, h)),
        )

    def chains(first, second, fin_first, fin_second):
        for hop in range(max(ny, nz) // 2):
            if hop > 0:
                prepare(first, hop)
                prepare(second, hop)
            go([first, second], hop)
        prepare_final(first, fin_first)
        prepare_final(second, fin_second)
        finish(first, fin_first)
        finish(second, fin_second)

    def each(body):
        for i in range(max(len(xz), len(xy))):
            for which, pairs in enumerate((xz, xy)):
                if i < len(pairs):
                    body(which, *pairs[i])

    @pl.when(c == U)
    def _():
        whole(rx_u.at[used], d_r).wait_recv()
        chains("uy", "uz", fin_uy, fin_uz)

        def send(which, dx, d):
            for to in (V, U):
                if (dx, d, to) != (0, 0, U):
                    send_u(dx, d, to)[which].start()

        each(send)
        r2_uy[col] = src_y(fin_uy, 0, 0)[U]
        r2_uz[here_z] = src_z(fin_uz, 0, 0)[U]
        whole(rx_d.at[used], d_s).wait_send()
        whole(st_uy, ys).wait_send()
        whole(st_uz, zs).wait_send()

    @pl.when(c == V)
    def _():
        whole(last_o.at[pl.ds(1, 4)], t_r.at[1]).wait_recv()
        whole(rx_d.at[used], d_r).wait_recv()
        whole(rx_p.at[:, :, used], xp_r).wait_recv()
        chains("py", "pz", fin_py, fin_pz)

        def send(which, dx, d):
            if (dx, d) != (0, 0):
                send_p(dx, d)[which].start()

        each(send)

        @pl.when(h != V)
        def _():
            for copy in send_p(0, 0):
                copy.start()

        @pl.when(h == V)
        def _():
            r2_py[col] = src_y(fin_py, 0, 0)[...]
            r2_pz[here_z] = src_z(fin_pz, 0, 0)[...]

        whole(rx_u.at[used], d_s).wait_send()
        whole(st_py, ys).wait_send()
        whole(st_pz, zs).wait_send()

    whole(last_o.at[pl.ds(0, 3)], t_s).wait_send()
    whole(rx_p.at[0, :, used], xp_s).wait_send()

    finals = ((r2_uy, n_y, fs.at[0]), (r2_uz, n_z, fs.at[1]))

    def take(r2, sem, count, kept):
        pl.when(kept)(lambda: whole(r2.at[pl.ds(0, count - 1)], sem).wait_recv())
        pl.when(jnp.logical_not(kept))(lambda: whole(r2.at[pl.ds(0, count)], sem).wait_recv())

    def summed(values):
        values = list(values)
        while len(values) > 1:
            values = [a + b for a, b in zip(values[::2], values[1::2])] + values[len(values) // 2 * 2 :]
        return values[0]

    take(r2_uy, fuyr, n_y, c == U)
    out[0, 0:SUB, 0:LANES] = summed(r2_uy[k] for k in range(n_y))
    take(r2_uz, fuzr, n_z, c == U)
    out[0, 0:SUB, LANES:] = summed(r2_uz[k] for k in range(n_z))
    mine = (c == V) & (h == V)
    take(r2_py, fpyr, n_y // 2, mine)
    out[0, SUB:, 0:LANES] = summed(r2_py[(2 * i + c) * nz + d] for i in range(half_x) for d in range(nz))
    take(r2_pz, fpzr, n_z // 2, mine)
    out[0, SUB:, LANES:] = summed(r2_pz[(2 * i + c) * ny + d] for i in range(half_x) for d in range(ny))

    @pl.when(c == U)
    def _():
        for r2, n, sem in finals:
            whole(r2, sem).wait_send()
            whole(r2.at[pl.ds(0, n - 1)], sem).wait_send()

    @pl.when(c == V)
    def _():
        for r2, n, sem in finals:
            whole(r2.at[pl.ds(0, n - 1)], sem).wait_send()
            pl.when(h != V)(lambda: whole(r2.at[0], sem).wait_send())


def on_device(dims, lhat, ainv_anc, diag_inv, targets):
    nx, ny, nz = dims
    slots, height, width = lhat.shape
    f32 = jnp.float32
    dma = pltpu.SemaphoreType.DMA
    k_all = nx * nz
    my, mz = nx // 2 * (ny - 1), nx // 2 * (nz - 1)
    tile = (SUB, LANES)

    def vm(*lead):
        return pltpu.VMEM((*lead, *tile), f32)

    scratch = [
        pltpu.VMEM((slots, 2, height, width), f32),
        pltpu.VMEM(diag_inv.shape[1:], f32),
        pltpu.SMEM((slots,), jnp.int32),
        vm(slots + 2, 2, ny, 2, 2),
        vm(slots + 2, 2, ny, 2),
        vm(slots + 2, 2, ny),
        vm(2, 2, slots + 2, ny),
        pltpu.SMEM((k_all,), jnp.int32),
        pltpu.SMEM((5, k_all), jnp.int32),
        *[vm(2, my, nz, 2), vm(2, mz, ny, 2), vm(2, my, nz), vm(2, mz, ny)] * 2,
        *[vm(nx, nz, 2), vm(nx, ny, 2), vm(nx, nz), vm(nx, ny)],
        *[vm(k_all), vm(nx * ny)] * 2,
        dma((slots + 2,)),
        *[dma] * 5,
        dma((2,)),
        dma,
        dma((2, my)),
        dma,
        dma((2, mz)),
        dma((2,)),
        *[dma] * 4,
    ]
    return pl.pallas_call(
        functools.partial(kernel, dims, slots),
        out_shape=jax.ShapeDtypeStruct(diag_inv.shape, f32),
        in_specs=[pl.BlockSpec(memory_space=pltpu.HBM)] * 4,
        out_specs=pl.BlockSpec(memory_space=pltpu.VMEM),
        scratch_shapes=scratch,
        compiler_params=pltpu.CompilerParams(
            collective_id=0, has_side_effects=True
        ),
        name="selected_blocks",
    )(lhat, ainv_anc, diag_inv, targets.reshape(slots))


def solution(mesh, nz=8):
    dims = (mesh.shape["col"] // nz, mesh.shape["row"] // 2, nz)
    placed = (
        P(("row", "col"), None, None),
        P(("row", "col"), None, None),
        P("col", "row", None),
        P(("row", "col"), None),
    )
    return jax.shard_map(
        functools.partial(on_device, dims), mesh=mesh, in_specs=placed, out_specs=P("col", "row", None), check_vma=False
    )
```

```python
import functools

import jax
import jax.numpy as jnp
from jax import lax
from jax.experimental import pallas as pl
from jax.experimental.pallas import tpu as pltpu
from jax.sharding import PartitionSpec as P

MESH = pl.DeviceIdType.MESH
LANES = 128
SUB = 8
U, V = 0, 1


def split(x):
    hi = x.astype(jnp.bfloat16)
    lo = (x - hi.astype(jnp.float32)).astype(jnp.bfloat16)
    return hi, lo


def transposed_product(a, b):
    ah, al = split(a)
    bh, bl = split(b)
    left = jnp.concatenate([ah, ah, al], axis=0)
    right = jnp.concatenate([bh, bl, bh], axis=0)
    return lax.dot_general(left, right, (((0,), (0,)), ((), ())), preferred_element_type=jnp.float32)


def kernel(
    dims, slots,
    lhat, ainv, dinv, targets, out,
    both, fac, ids, prod, rx_u, rx_d, rx_p, last_a, last_o,
    st_uy, st_uz, st_py, st_pz, rc_uy, rc_uz, rc_py, rc_pz,
    fin_uy, fin_uz, fin_py, fin_pz, r2_uy, r2_uz, r2_py, r2_pz,
    in_sem, d_s, d_r, xp_s, xp_r, t_s, t_r,
    ys, yr, zs, zr, fs, fuyr, fuzr, fpyr, fpzr,
):
    nx, ny, nz = dims
    row, col = lax.axis_index("row"), lax.axis_index("col")
    y, c = row // 2, row % 2
    x, z = col // nz, col % nz
    h = x % 2
    none = slots + 1
    half_x = nx // 2

    def wrap(v, n):
        return jnp.where(v >= n, v - n, v)

    xs = [x] + [wrap(x + d, nx) for d in range(1, nx)]
    yy = [y] + [wrap(y + d, ny) for d in range(1, ny)]
    zz = [z] + [wrap(z + d, nz) for d in range(1, nz)]

    def at(xv, yv, zv, cv):
        return (yv * 2 + cv, xv * nz + zv)

    partner = at(x, y, z, 1 - c)
    pair_y = jnp.where(h == 0, xs[1], xs[nx - 1])
    pair_z = jnp.where(h == 0, xs[nx - 1], xs[1])

    def remote(src, dst, ss, rs, device):
        return pltpu.make_async_remote_copy(src, dst, ss, rs, device_id=device, device_id_type=MESH)

    def loads(s):
        return (
            pltpu.make_async_copy(lhat.at[s], both.at[s, 0], in_sem.at[s]),
            pltpu.make_async_copy(ainv.at[s], both.at[s, 1], in_sem.at[s]),
        )

    fac_load = pltpu.make_async_copy(dinv.at[0], fac, in_sem.at[slots])
    ids_load = pltpu.make_async_copy(targets, ids, in_sem.at[slots + 1])
    ids_load.start()
    fac_load.start()
    for s in range(slots):
        for load in loads(s):
            load.start()

    barrier = pltpu.get_barrier_semaphore()
    peers = [partner, at(x, yy[1], z, c), at(x, yy[ny - 1], z, c), at(x, y, zz[1], c), at(x, y, zz[nz - 1], c)]
    for d in range(1, nx):
        peers += [at(xs[d], y, z, c), at(xs[d], y, z, 1 - c)]
    for peer in peers:
        pl.semaphore_signal(barrier, inc=1, device_id=peer, device_id_type=MESH)

    prod[none] = jnp.zeros(prod.shape[1:], jnp.float32)
    rx_u[none] = jnp.zeros(rx_u.shape[1:], jnp.float32)
    rx_d[none] = jnp.zeros(rx_d.shape[1:], jnp.float32)
    for i in range(2):
        for j in range(2):
            rx_p[i, j, none] = jnp.zeros(rx_p.shape[3:], jnp.float32)

    def put(s, value, before):
        for i in range(2):
            part = value[:, i * LANES : (i + 1) * LANES].reshape(prod.shape[2:])
            prod[s, i] = part if before is None else prod[before, i] - part

    ids_load.wait()

    def table(k, carry):
        found = jnp.where(col == k, 0, none)
        for s in range(slots):
            found = jnp.where(ids[s] == k, s + 1, found)
        last_a[k] = found
        return carry

    lax.fori_loop(0, nx * nz, table, 0)
    fac_load.wait()
    put(0, transposed_product(fac[...], fac[...]), None)
    pl.semaphore_wait(barrier, len(peers))

    to_py = at(pair_y, y, z, V)
    to_pz = at(pair_z, y, z, V)
    tables = [
        remote(last_a, last_o.at[0], t_s, t_r.at[0], partner),
        remote(last_a, last_o.at[1 + c], t_s, t_r.at[1], to_py),
        remote(last_a, last_o.at[3 + c], t_s, t_r.at[1], to_pz),
    ]
    for copy in tables:
        copy.start()

    def across(s):
        return (
            remote(prod.at[s, 0, :, 1 - h, 1], rx_p.at[0, c, s], xp_s, xp_r, to_py),
            remote(prod.at[s, 1, :, 1 - h, 1], rx_p.at[1, c, s], xp_s, xp_r, to_pz),
        )

    def exchange(s):
        @pl.when(c == U)
        def _():
            remote(prod.at[s, :, :, h, 1], rx_d.at[s], d_s, d_r, partner).start()

        @pl.when(c == V)
        def _():
            remote(prod.at[s, :, :, :, 0], rx_u.at[s], d_s, d_r, partner).start()

        for copy in across(s):
            copy.start()

    for s in range(slots):
        pltpu.make_async_copy(both.at[s], both.at[s], in_sem.at[s]).wait()
        value = transposed_product(both[s, 0], both[s, 1])
        before = jnp.where(ids[s] == col, 0, none)
        for e in range(s):
            before = jnp.where(ids[e] == ids[s], e + 1, before)
        put(s + 1, value, before)
        exchange(s)
    exchange(slots)

    def local_uy(k, yb):
        return prod[last_a[k], 0, yb, :, 0] + rx_u[last_o[0, k], 0, yb]

    def local_uz(k):
        return prod[last_a[k], 1, :, :, 0] + rx_u[last_o[0, k], 1]

    def local_py(k, yb):
        own = prod[last_a[k], 0, yb, h, 1] + rx_d[last_o[0, k], 0, yb]
        return own + (rx_p[0, 0, last_o[1, k], yb] + rx_p[0, 1, last_o[2, k], yb])

    def local_pz(k):
        own = prod[last_a[k], 1, :, h, 1] + rx_d[last_o[0, k], 1]
        return own + (rx_p[1, 0, last_o[3, k]] + rx_p[1, 1, last_o[4, k]])

    parts = {
        "uy": (st_uy, rc_uy, ys, yr, local_uy, ny, yy),
        "uz": (st_uz, rc_uz, zs, zr, local_uz, nz, zz),
        "py": (st_py, rc_py, ys, yr, local_py, ny, yy),
        "pz": (st_pz, rc_pz, zs, zr, local_pz, nz, zz),
    }

    def place_of(which, way, q, hop):
        n = parts[which][5]
        long = (q < half_x) == (way == 0)
        hops = n // 2 if long else n // 2 - 1
        base = (q % half_x) * hops + (0 if long else half_x * (n // 2))
        return hops, base + hop

    def message(which, way, m):
        st, rc, ss, rs, _, n, at_axis = parts[which]
        to = at_axis[1 if way == 0 else n - 1]
        device = at(x, to, z, c) if which[1] == "y" else at(x, y, to, c)
        return remote(st.at[way, m], rc.at[way, m], ss, rs.at[way, m], device)

    def terms(which, q, dest, dst):
        local = parts[which][4]
        if which[1] == "y":
            for i in range(nz):
                dst[i] = local(q * nz + i, dest)
        else:
            dst[...] = local(q * nz + dest)

    def flows(which, hop):
        for late in (0, 1):
            for j in range(half_x):
                for way in (0, 1):
                    q = (way if late == 0 else 1 - way) * half_x + j
                    hops, m = place_of(which, way, q, hop)
                    if hop < hops:
                        yield way, q, hops, m

    def own(which, hop, way, q, hops, m):
        st, _, _, _, _, n, at_axis = parts[which]
        dest = at_axis[(hops - hop) % n if way == 0 else (n - hops + hop) % n]
        terms(which, q, dest, st.at[way, m])

    def prepare(which, hop):
        for flow in flows(which, hop):
            own(which, hop, *flow)

    def go(whiches, hop):
        lists = [[(w, f) for f in flows(w, hop)] for w in whiches]
        for i in range(max(len(found) for found in lists)):
            for found in lists:
                if i >= len(found):
                    continue
                which, (way, q, hops, m) = found[i]
                st, rc = parts[which][0], parts[which][1]
                if hop == 0:
                    own(which, hop, way, q, hops, m)
                else:
                    message(which, way, m - 1).wait_recv()
                    st[way, m] = st[way, m] + rc[way, m - 1]
                message(which, way, m).start()

    def finish(which, fin):
        _, rc, _, _, _, n, at_axis = parts[which]
        for q in range(nx):
            for way in (0, 1):
                hops, m = place_of(which, way, q, 0)
                if hops == 0:
                    continue
                m = m + hops - 1
                message(which, way, m).wait_recv()
                fin[q] = fin[q] + rc[way, m]

    def prepare_final(which, fin):
        for q in range(nx):
            terms(which, q, parts[which][6][0], fin.at[q])

    used = pl.ds(0, slots + 1)

    def whole(ref, sem):
        return remote(ref, ref, sem, sem, partner)

    tables[0].wait_recv()

    def far(d, n):
        return min(d, n - d)

    xz = sorted(((dx, dz) for dx in range(nx) for dz in range(nz)), key=lambda p: -far(p[0], nx) - far(p[1], nz))
    xy = sorted(((dx, dy) for dx in range(nx) for dy in range(ny)), key=lambda p: -far(p[0], nx) - far(p[1], ny))
    here_z = x * ny + y

    def src_y(fin, dx, dz):
        return fin.at[xs[dx], zz[dz]]

    def src_z(fin, dx, dy):
        return fin.at[xs[dx], yy[dy]]

    n_y, n_z = nx * nz, nx * ny

    def send_u(dx, d, to):
        return (
            remote(src_y(fin_uy, dx, d).at[to], r2_uy.at[col], fs.at[0], fuyr, at(xs[dx], y, zz[d], to)),
            remote(src_z(fin_uz, dx, d).at[to], r2_uz.at[here_z], fs.at[1], fuzr, at(xs[dx], yy[d], z, to)),
        )

    def send_p(dx, d):
        return (
            remote(src_y(fin_py, dx, d), r2_py.at[col], fs.at[0], fpyr, at(xs[dx], y, zz[d], h)),
            remote(src_z(fin_pz, dx, d), r2_pz.at[here_z], fs.at[1], fpzr, at(xs[dx], yy[d], z, h)),
        )

    def chains(first, second, fin_first, fin_second):
        for hop in range(max(ny, nz) // 2):
            go([first, second], hop)
            if hop == 0:
                for later in range(1, max(ny, nz) // 2):
                    prepare(first, later)
                    prepare(second, later)
                prepare_final(first, fin_first)
                prepare_final(second, fin_second)
        finish(first, fin_first)
        finish(second, fin_second)

    def each(body):
        for i in range(max(len(xz), len(xy))):
            for which, pairs in enumerate((xz, xy)):
                if i < len(pairs):
                    body(which, *pairs[i])

    @pl.when(c == U)
    def _():
        whole(rx_u.at[used], d_r).wait_recv()
        chains("uy", "uz", fin_uy, fin_uz)

        def send(which, dx, d):
            for to in (V, U):
                if (dx, d, to) != (0, 0, U):
                    send_u(dx, d, to)[which].start()

        each(send)
        r2_uy[col] = src_y(fin_uy, 0, 0)[U]
        r2_uz[here_z] = src_z(fin_uz, 0, 0)[U]
        whole(rx_d.at[used], d_s).wait_send()
        whole(st_uy, ys).wait_send()
        whole(st_uz, zs).wait_send()

    @pl.when(c == V)
    def _():
        whole(last_o.at[pl.ds(1, 4)], t_r.at[1]).wait_recv()
        whole(rx_d.at[used], d_r).wait_recv()
        whole(rx_p.at[:, :, used], xp_r).wait_recv()
        chains("py", "pz", fin_py, fin_pz)

        def send(which, dx, d):
            if (dx, d) != (0, 0):
                send_p(dx, d)[which].start()

        each(send)

        @pl.when(h != V)
        def _():
            for copy in send_p(0, 0):
                copy.start()

        @pl.when(h == V)
        def _():
            r2_py[col] = src_y(fin_py, 0, 0)[...]
            r2_pz[here_z] = src_z(fin_pz, 0, 0)[...]

        whole(rx_u.at[used], d_s).wait_send()
        whole(st_py, ys).wait_send()
        whole(st_pz, zs).wait_send()

    whole(last_o.at[pl.ds(0, 3)], t_s).wait_send()
    whole(rx_p.at[0, :, used], xp_s).wait_send()

    finals = ((r2_uy, n_y, fs.at[0]), (r2_uz, n_z, fs.at[1]))

    def take(r2, sem, count, kept):
        pl.when(kept)(lambda: whole(r2.at[pl.ds(0, count - 1)], sem).wait_recv())
        pl.when(jnp.logical_not(kept))(lambda: whole(r2.at[pl.ds(0, count)], sem).wait_recv())

    def summed(values):
        values = list(values)
        while len(values) > 1:
            values = [a + b for a, b in zip(values[::2], values[1::2])] + values[len(values) // 2 * 2 :]
        return values[0]

    mine = (c == V) & (h == V)
    take(r2_py, fpyr, n_y // 2, mine)
    out[0, SUB:, 0:LANES] = summed(r2_py[(2 * i + c) * nz + d] for i in range(half_x) for d in range(nz))
    take(r2_pz, fpzr, n_z // 2, mine)
    out[0, SUB:, LANES:] = summed(r2_pz[(2 * i + c) * ny + d] for i in range(half_x) for d in range(ny))
    take(r2_uy, fuyr, n_y, c == U)
    out[0, 0:SUB, 0:LANES] = summed(r2_uy[k] for k in range(n_y))
    take(r2_uz, fuzr, n_z, c == U)
    out[0, 0:SUB, LANES:] = summed(r2_uz[k] for k in range(n_z))

    @pl.when(c == U)
    def _():
        for r2, n, sem in finals:
            whole(r2, sem).wait_send()
            whole(r2.at[pl.ds(0, n - 1)], sem).wait_send()

    @pl.when(c == V)
    def _():
        for r2, n, sem in finals:
            whole(r2.at[pl.ds(0, n - 1)], sem).wait_send()
            pl.when(h != V)(lambda: whole(r2.at[0], sem).wait_send())


def on_device(dims, lhat, ainv_anc, diag_inv, targets):
    nx, ny, nz = dims
    slots, height, width = lhat.shape
    f32 = jnp.float32
    dma = pltpu.SemaphoreType.DMA
    k_all = nx * nz
    my, mz = nx // 2 * (ny - 1), nx // 2 * (nz - 1)
    tile = (SUB, LANES)

    def vm(*lead):
        return pltpu.VMEM((*lead, *tile), f32)

    scratch = [
        pltpu.VMEM((slots, 2, height, width), f32),
        pltpu.VMEM(diag_inv.shape[1:], f32),
        pltpu.SMEM((slots,), jnp.int32),
        vm(slots + 2, 2, ny, 2, 2),
        vm(slots + 2, 2, ny, 2),
        vm(slots + 2, 2, ny),
        vm(2, 2, slots + 2, ny),
        pltpu.SMEM((k_all,), jnp.int32),
        pltpu.SMEM((5, k_all), jnp.int32),
        *[vm(2, my, nz, 2), vm(2, mz, ny, 2), vm(2, my, nz), vm(2, mz, ny)] * 2,
        *[vm(nx, nz, 2), vm(nx, ny, 2), vm(nx, nz), vm(nx, ny)],
        *[vm(k_all), vm(nx * ny)] * 2,
        dma((slots + 2,)),
        *[dma] * 5,
        dma((2,)),
        dma,
        dma((2, my)),
        dma,
        dma((2, mz)),
        dma((2,)),
        *[dma] * 4,
    ]
    return pl.pallas_call(
        functools.partial(kernel, dims, slots),
        out_shape=jax.ShapeDtypeStruct(diag_inv.shape, f32),
        in_specs=[pl.BlockSpec(memory_space=pltpu.HBM)] * 4,
        out_specs=pl.BlockSpec(memory_space=pltpu.VMEM),
        scratch_shapes=scratch,
        compiler_params=pltpu.CompilerParams(
            collective_id=0, has_side_effects=True
        ),
        name="selected_blocks",
    )(lhat, ainv_anc, diag_inv, targets.reshape(slots))


def solution(mesh, nz=8):
    dims = (mesh.shape["col"] // nz, mesh.shape["row"] // 2, nz)
    placed = (
        P(("row", "col"), None, None),
        P(("row", "col"), None, None),
        P("col", "row", None),
        P(("row", "col"), None),
    )
    return jax.shard_map(
        functools.partial(on_device, dims), mesh=mesh, in_specs=placed, out_specs=P("col", "row", None), check_vma=False
    )
```
